128 devices in a mesh: seq: 32 (over z_hi, x, y), head: 4 (over z_lo, core).
Axes of the slice: x: 4, y: 4, z: 4 (z_hi: 2, z_lo: 2; z = z_hi * 2 + z_lo), core: 2. Of those that a mesh axis runs over, the one named last changes fastest.
Arguments:
- latent: bfloat16 [4096, 1024], P('seq'), may hold values from -15 to 15
- probe: bfloat16 [4096, 1024], P('seq'), may hold values from -6 to 6
- time_embed: float32 [1024], replicated, may hold values from -6 to 6
- gain_attn: float32 [1024], replicated, may hold values from 0.1 to 1.9
- w_query: bfloat16 [1024, 1024], P(None, 'head'), may hold values from -0.625 to 0.625
- w_key: bfloat16 [1024, 1024], P(None, 'head'), may hold values from -11 to 11
- w_value: bfloat16 [1024, 1024], P(None, 'head'), may hold values from -0.1875 to 0.1875
- w_out: bfloat16 [1024, 1024], P('head'), may hold values from -0.1875 to 0.1875
- gain_mlp: float32 [1024], replicated, may hold values from 0.1 to 1.9
- w_in: bfloat16 [1024, 4096], P(None, 'head'), may hold values from -0.1875 to 0.1875
- w_down: bfloat16 [4096, 1024], P('head'), may hold values from -0.09375 to 0.09375
Outputs:
- latent_end: float32 [4096, 1024], P('seq')
- frame_trace: float32 [4096], P('seq')
- frame_logp: float32 [4096], P('seq')
- mean_logp: float32 [], replicated
The draws below stay inside these ranges and needn't reach their ends.
All inputs are finite; a program needn't handle non-finite values.
Results may differ from the reference program's by a relative error of at most 0.03.
The reference program's roundings to bfloat16 on the way count: a program that leaves them out, or rounds other values in their place, can miss the bound.
Values may be sent and summed in bfloat16 or wider, within the bound.
A program may use at most 64 MiB of HBM per device.

```python
import math
import jax
import jax.numpy as jnp
from jax import lax

D = 1024
HEADS = 16
HEAD_DIM = 64
FF = 4096
STEPS = 2
FRAMES = 4096


def weight_pair(key):
    base = jax.random.fold_in(key, 11)
    first, second = jax.random.split(base, 2)
    query_weight = jnp.clip(jax.random.normal(first, (D, D), jnp.float32), -5.0, 5.0) * D ** (-0.5)
    noise = jnp.clip(jax.random.normal(second, (D, D), jnp.float32), -5.0, 5.0) * D ** (-0.5)
    key_weight = 3.0 * noise
    return (query_weight, key_weight)


def draw_w_query(key, part):
    return weight_pair(key)[0].astype(jnp.bfloat16)


def draw_w_key(key, part):
    return weight_pair(key)[1].astype(jnp.bfloat16)


def draw_latent(key, part):
    base = jax.random.fold_in(key, 23)
    position = jnp.arange(FRAMES, dtype=jnp.float32) / max(FRAMES - 1, 1)
    entries = jnp.clip(jax.random.normal(base, (FRAMES, D), jnp.float32), -5.0, 5.0)
    ramp = 1.0 + 2.0 * position
    return (entries * ramp[:, None]).astype(jnp.bfloat16)


def steps_of(key, extent, shards, low, high):
    factor_of, own = 1.0, jax.random.fold_in(key, 6)
    for dim, blocks in shards:
        heights = jnp.exp(jax.random.uniform(jax.random.fold_in(own, dim), (blocks,), jnp.float32, low / len(shards), high / len(shards)))
        factor_of = factor_of * jnp.repeat(heights, extent[dim] // blocks).reshape([-1 if axis == dim else 1 for axis in range(len(extent))])
    return factor_of


def normal_values(stream_key, extent, deviation, most, shards=(), held_as=jnp.bfloat16):
    array = jax.random.normal(stream_key, extent, jnp.float32) * deviation
    if len(shards) > 0:
        array = steps_of(stream_key, extent, shards, -0.22, 0.18) * array
    return jnp.clip(array, min=-most, max=most).astype(held_as)


def setup_inputs(seed: int = 0) -> dict:
    key_of = jax.random.split(jax.random.key(seed), 12)
    latent = draw_latent(jax.random.fold_in(key_of[11], 71), 0)
    probe = normal_values(key_of[1], (FRAMES, D), 1.0, 6.0, ((0, 32),))
    time_embed = normal_values(key_of[2], (D,), 1.0, 6.0, (), jnp.float32)
    gain_attn = jnp.clip(1.0 + 0.18 * jax.random.normal(key_of[3], (D,), jnp.float32), 0.1, 1.9)
    w_query = draw_w_query(jax.random.fold_in(key_of[11], 71), 0)
    w_key = draw_w_key(jax.random.fold_in(key_of[11], 71), 0)
    w_value = normal_values(key_of[6], (D, D), D ** -0.5, 0.1875, ((1, 4),))
    w_out = normal_values(key_of[7], (D, D), D ** -0.5, 0.1875, ((0, 4),))
    gain_mlp = jnp.clip(1.0 + 0.18 * jax.random.normal(key_of[8], (D,), jnp.float32), 0.1, 1.9)
    w_in = normal_values(key_of[9], (D, FF), D ** -0.5, 0.1875, ((1, 4),))
    w_down = normal_values(key_of[10], (FF, D), FF ** -0.5, 0.09375, ((0, 4),))
    return dict(latent=latent, probe=probe, time_embed=time_embed, gain_attn=gain_attn, w_query=w_query, w_key=w_key, w_value=w_value, w_out=w_out, gain_mlp=gain_mlp, w_in=w_in, w_down=w_down)


EPSILON = 1e-05
GELU_COEF = 0.044715
ROOT_TWO_PI = math.sqrt(2.0 / math.pi)

def norm_pair(values, tangent, norm_gain):
    meansq = lax.optimization_barrier(jnp.mean(values * values, axis=-1, keepdims=True)) + EPSILON
    inverse = lax.rsqrt(meansq)
    inner_mean = lax.optimization_barrier(jnp.mean(values * tangent, axis=-1, keepdims=True))
    primal = values * inverse * norm_gain
    derived = (tangent * inverse - values * inverse ** 3 * inner_mean) * norm_gain
    return (primal.astype(jnp.bfloat16), derived.astype(jnp.bfloat16))

def gelu_pair(pre_act, tangent):
    cubic_arg = pre_act + GELU_COEF * pre_act ** 3
    tanh_value = jnp.tanh(ROOT_TWO_PI * cubic_arg)
    output = 0.5 * pre_act * (1.0 + tanh_value)
    slope_value = 0.5 * (1.0 + tanh_value) + 0.5 * pre_act * (1.0 - tanh_value * tanh_value) * ROOT_TWO_PI * (1.0 + 3.0 * GELU_COEF * pre_act * pre_act)
    return (output.astype(jnp.bfloat16), (slope_value * tangent).astype(jnp.bfloat16))

def attention(queries, query_tang, keys, vals, key_tang, val_tang):
    scale = HEAD_DIM ** (-0.5)

    def heads_of(matrix):
        return matrix.astype(jnp.float32).reshape(FRAMES, HEADS, HEAD_DIM)
    keys_all = heads_of(keys)
    vals_all = heads_of(vals)
    key_tang_all = heads_of(key_tang)
    val_tang_all = heads_of(val_tang)
    block = math.gcd(FRAMES, 512)

    def one_block(pair):
        block_queries, block_tang = pair
        scores = jnp.einsum('bhd,shd->hbs', block_queries, keys_all) * scale
        score_tang = (jnp.einsum('bhd,shd->hbs', block_tang, keys_all) + jnp.einsum('bhd,shd->hbs', block_queries, key_tang_all)) * scale
        row_top = lax.optimization_barrier(jnp.max(scores, axis=-1, keepdims=True))
        weights = jnp.exp(scores - row_top)
        total = lax.optimization_barrier(jnp.sum(weights, axis=-1))
        weighted = weights * score_tang
        carried = lax.optimization_barrier(jnp.sum(weighted, axis=-1))
        rounded = lax.optimization_barrier(weights.astype(jnp.bfloat16)).astype(jnp.float32)
        rounded_tang = lax.optimization_barrier(weighted.astype(jnp.bfloat16)).astype(jnp.float32)
        acc_primal = jnp.einsum('hbs,shd->bhd', rounded, vals_all)
        acc_tang = jnp.einsum('hbs,shd->bhd', rounded_tang, vals_all) + jnp.einsum('hbs,shd->bhd', rounded, val_tang_all)
        total_t = jnp.transpose(total)[:, :, None]
        carried_t = jnp.transpose(carried)[:, :, None]
        primal = acc_primal / total_t
        tangent = acc_tang / total_t - carried_t / total_t * primal
        return (primal.astype(jnp.bfloat16), tangent.astype(jnp.bfloat16))
    query_blocks = heads_of(queries).reshape(FRAMES // block, block, HEADS, HEAD_DIM)
    tang_blocks = heads_of(query_tang).reshape(FRAMES // block, block, HEADS, HEAD_DIM)
    head_out, head_tang = lax.map(one_block, (query_blocks, tang_blocks))
    return (head_out.reshape(FRAMES, D), head_tang.reshape(FRAMES, D))

def vector_field(inputs, direction, gain_attn, w_query, w_key, w_value, w_out, gain_mlp, w_in, w_down):
    normed, normed_tang = norm_pair(inputs, direction, gain_attn)

    def project(weight):
        primal = jnp.dot(normed, weight, preferred_element_type=jnp.float32).astype(jnp.bfloat16)
        tangent = jnp.dot(normed_tang, weight, preferred_element_type=jnp.float32).astype(jnp.bfloat16)
        return (primal, tangent)
    queries, query_tang = project(w_query)
    keys, key_tang = project(w_key)
    vals, val_tang = project(w_value)
    head_out, head_tang = attention(queries, query_tang, keys, vals, key_tang, val_tang)
    attn = jnp.dot(head_out, w_out, preferred_element_type=jnp.float32)
    attn_tang = jnp.dot(head_tang, w_out, preferred_element_type=jnp.float32)
    middle = inputs + attn
    middle_tang = direction + attn_tang
    normed_mlp, normed_mlp_tang = norm_pair(middle, middle_tang, gain_mlp)
    pre_act = jnp.dot(normed_mlp, w_in, preferred_element_type=jnp.float32)
    pre_tang = jnp.dot(normed_mlp_tang, w_in, preferred_element_type=jnp.float32)
    activ, activ_tang = gelu_pair(pre_act, pre_tang)
    mlp_out = jnp.dot(activ, w_down, preferred_element_type=jnp.float32)
    mlp_tang = jnp.dot(activ_tang, w_down, preferred_element_type=jnp.float32)
    return (attn + mlp_out, attn_tang + mlp_tang)

def reference(latent, probe, time_embed, gain_attn, w_query, w_key, w_value, w_out, gain_mlp, w_in, w_down):
    state = latent.astype(jnp.float32)
    direction = probe.astype(jnp.float32)
    trace = jnp.zeros((FRAMES,), jnp.float32)
    for euler_step in range(STEPS):
        inputs = state + euler_step / STEPS * time_embed
        field, field_tang = vector_field(inputs, direction, gain_attn, w_query, w_key, w_value, w_out, gain_mlp, w_in, w_down)
        trace = trace + lax.optimization_barrier(jnp.sum(direction * field_tang, axis=-1)) / (STEPS * D)
        state = state + field / STEPS
    frame_logp = trace - 0.5 * lax.optimization_barrier(jnp.sum(state * state, axis=-1)) / D - 0.5 * math.log(2.0 * math.pi)
    mean_logp = jnp.mean(frame_logp)
    return (state, trace, frame_logp, mean_logp)
```

```python
import functools
import math

import jax
import jax.numpy as jnp
from jax import lax
from jax.experimental import pallas as pl
from jax.experimental.pallas import tpu as pltpu
from jax.sharding import PartitionSpec as P

HEAD_DIM = 64
STEPS = 2
EPSILON = 1e-05
GELU_COEF = 0.044715
ROOT_TWO_PI = math.sqrt(2.0 / math.pi)

ROWS = 64
SEQ_ROWS = 128
WIDTH = 1024
RING = 4
QROWS = 512
NEG = -1e30

OWN, LEFT, RIGHT, FAR, ZOWN, ZLEFT, ZRIGHT, ZFAR = range(8)

f32 = jnp.float32
bf16 = jnp.bfloat16


def norm_pair(values, tangent, norm_gain):
    meansq = jnp.mean(values * values, axis=-1, keepdims=True) + EPSILON
    inverse = lax.rsqrt(meansq)
    inner_mean = jnp.mean(values * tangent, axis=-1, keepdims=True)
    primal = values * inverse * norm_gain
    derived = (tangent * inverse - values * inverse**3 * inner_mean) * norm_gain
    return jnp.concatenate([primal.astype(bf16), derived.astype(bf16)], axis=0)


def gelu_pair(pre_act, tangent):
    cubic_arg = pre_act + GELU_COEF * pre_act * pre_act * pre_act
    tanh_value = jnp.tanh(ROOT_TWO_PI * cubic_arg)
    output = 0.5 * pre_act * (1.0 + tanh_value)
    slope_value = 0.5 * (1.0 + tanh_value) + 0.5 * pre_act * (
        1.0 - tanh_value * tanh_value
    ) * ROOT_TWO_PI * (1.0 + 3.0 * GELU_COEF * pre_act * pre_act)
    return (output.astype(bf16), (slope_value * tangent).astype(bf16))


def swap_halves(tile):
    return pltpu.roll(tile, HEAD_DIM, 1)


def kernel(
    latent, probe, time_embed, gain_attn, w_query, w_key, w_value, w_out, gain_mlp, w_in, w_down,
    o_state, o_trace, o_logp, o_mean,
    lat_in, prb_in, wq, wk, wv, wo, wi, wd,
    state, direction, inputs_s, trace_s, attn_s, normed_s, act_s,
    stage_kv, stage_q, kv, qin, q1, q2, relay, acc_p, acc_t, top_s, total_s, carried_s,
    ret_stage, ret, red_send, red_recv, stat_mine, stat_in, mean_send, mean_recv,
    load_sem, wsend, wrecv, kv_send, kv_recv, q_send, q_recv, self_sem, g_send, g_recv, r_recv,
    ret_send, ret_recv, red_ssem, red_rsem, fin_send, fin_recv, mean_ssem, mean_rsem,
):
    s = lax.axis_index("seq")
    hd = lax.axis_index("head")
    x = lax.rem(s // 4, 4)
    y = lax.rem(s, 4)
    c = lax.rem(hd, 2)
    other = 1 - c
    zlo = hd // 2
    z = (s // 16) * 2 + zlo
    a = y + c * (x - y)
    g = x + c * (y - x)

    def place(aa, gg, zz, cc):
        aa, gg, zz = lax.rem(aa, 4), lax.rem(gg, 4), lax.rem(zz, 4)
        xx = gg + c * (aa - gg)
        yy = aa + c * (gg - aa)
        return ((zz // 2) * 16 + xx * 4 + yy, lax.rem(zz, 2) * 2 + cc)

    def remote(src, dst, ssem, rsem, where):
        return pltpu.make_async_remote_copy(
            src_ref=src, dst_ref=dst, send_sem=ssem, recv_sem=rsem,
            device_id=where, device_id_type=pl.DeviceIdType.MESH,
        )

    here = place(a, g, z, other)
    zn = z + 1 + 2 * c
    zpair = z + 1 - 2 * zlo

    barrier = pltpu.get_barrier_semaphore()
    greeted = (
        [place(a + d, g, z, c) for d in (1, 2, 3)]
        + [place(a + d, g, z, other) for d in range(4)]
        + [place(a, g + d, z, other) for d in (1, 2, 3)]
        + [place(a, g + d, z, c) for d in (1, 2, 3)]
        + [place(a, g, z + d, c) for d in (1, 2, 3)]
    )
    for where in greeted:
        pl.semaphore_signal(
            barrier, inc=1, device_id=where, device_id_type=pl.DeviceIdType.MESH
        )

    row0 = pl.multiple_of(c * ROWS, ROWS)
    loads = [
        pltpu.make_async_copy(latent.at[pl.ds(row0, ROWS)], lat_in, load_sem.at[0]),
        pltpu.make_async_copy(probe.at[pl.ds(row0, ROWS)], prb_in, load_sem.at[1]),
    ]
    weights = [(w_query, wq), (w_key, wk), (w_value, wv), (w_out, wo), (w_in, wi), (w_down, wd)]
    for i, (src, dst) in enumerate(weights):
        loads.append(pltpu.make_async_copy(src, dst.at[c], load_sem.at[2 + i]))
    for load in loads:
        load.start()
    pl.semaphore_wait(barrier, len(greeted))
    swaps = [
        remote(src, dst.at[c], wsend.at[i], wrecv.at[i], here)
        for i, (src, dst) in enumerate(weights)
    ]
    for swap in swaps:
        swap.start()

    loads[0].wait()
    loads[1].wait()
    state[...] = lat_in[...].astype(f32)
    direction[...] = prb_in[...].astype(f32)
    trace_s[...] = jnp.zeros_like(trace_s)

    lane = lax.broadcasted_iota(jnp.int32, (ROWS, 128), 1)
    low = lane < HEAD_DIM
    low_c = lax.broadcasted_iota(jnp.int32, (128, 128), 1) < HEAD_DIM

    def weights_here(i):
        loads[2 + i].wait()
        swaps[i].wait()

    for i in range(6):
        weights_here(i)

    def one_step(t, carry):
        inputs = state[...] + (t.astype(f32) / STEPS) * time_embed[...]
        inputs_s[...] = inputs
        normed_s[...] = norm_pair(inputs, direction[...], gain_attn[...])
        normed = normed_s[...]

        for cc in range(2):
            for which, weight in enumerate((wk, wv, wq)):
                both = jnp.dot(normed, weight[cc], preferred_element_type=f32)
                if which == 2:
                    both = both * (HEAD_DIM**-0.5)
                for j in range(2):
                    prim = both[:ROWS, j * 128 : (j + 1) * 128]
                    tang = both[ROWS:, j * 128 : (j + 1) * 128]
                    first = jnp.where(low, prim, swap_halves(tang)).astype(bf16)
                    second = jnp.where(low, swap_halves(prim), tang).astype(bf16)
                    if which == 2:
                        stage_q[t, cc, 2 * j] = first
                        stage_q[t, cc, 2 * j + 1] = second
                    else:
                        stage_kv[t, cc, 2 * j, :, which * 128 : (which + 1) * 128] = first
                        stage_kv[t, cc, 2 * j + 1, :, which * 128 : (which + 1) * 128] = second

        def kv_slot(slot, kind):
            return kv.at[t, OWN, pl.ds((slot * 2 + kind) * ROWS, ROWS)]

        def q_slot(slot, kind):
            return qin.at[t, slot * 2 + kind]

        kv_out, q_out = [], []
        for d in (0, 1, 3, 2):
            slot = (4 - d) % 4
            for kind in (1, 0):
                if kind == 0 and d == 0:
                    continue
                if kind == 0:
                    cc, to, head = c, place(a + d, g, z, c), lax.rem(a + d, 4)
                else:
                    cc, to, head = other, place(a, g + d, z, other), lax.rem(g + d, 4)
                n = slot * 2 + kind
                kv_out.append(remote(
                    stage_kv.at[t, cc, head], kv_slot(slot, kind),
                    kv_send.at[t, n], kv_recv.at[t, n], to,
                ))
                q_out.append(remote(
                    stage_q.at[t, cc, head], q_slot(slot, kind),
                    q_send.at[t, n], q_recv.at[t, n], to,
                ))
        for copy in kv_out:
            copy.start()
        for copy in q_out:
            copy.start()
        kv_self = pltpu.make_async_copy(stage_kv.at[t, c, a], kv_slot(0, 0), self_sem.at[0])
        q_self = pltpu.make_async_copy(stage_q.at[t, c, a], q_slot(0, 0), self_sem.at[1])
        kv_self.start()
        q_self.start()

        def piece(block, p):
            return kv.at[t, block, pl.ds(p * 128, 128)]

        sent = []

        def send(src, block, p, to):
            n = len(sent)
            copy = remote(src, piece(block, p), g_send.at[t, n], g_recv.at[t, block, p], to)
            copy.start()
            sent.append(copy)

        right, left = place(a, g + 1, z, c), place(a, g + 3, z, c)
        onward = place(a, g, zn, c)

        def arrived(block, p):
            remote(
                piece(block, p), piece(block, p), g_send.at[t, 0], g_recv.at[t, block, p], right
            ).wait_recv()

        for slot in (0, 1, 3, 2):
            for kind in range(2):
                if slot == 0 and kind == 0:
                    kv_self.wait()
                else:
                    n = slot * 2 + kind
                    remote(
                        kv_slot(slot, kind), kv_slot(slot, kind), kv_send.at[t, n],
                        kv_recv.at[t, n], right,
                    ).wait_recv()
            send(piece(OWN, slot), LEFT, slot, right)
            send(piece(OWN, slot), RIGHT, slot, left)
            n = len(sent)
            copy = remote(
                piece(OWN, slot), relay.at[t, pl.ds(slot * 128, 128)], g_send.at[t, n],
                r_recv.at[t, slot], onward,
            )
            copy.start()
            sent.append(copy)

        for n in range(8):
            if n == 0:
                q_self.wait()
            else:
                remote(
                    qin.at[t, n], qin.at[t, n], q_send.at[t, n], q_recv.at[t, n], right
                ).wait_recv()

        def prepare(n, carry):
            tile = qin[t, n].astype(f32)
            q1[pl.ds(n * ROWS, ROWS), :] = jnp.where(low, tile, 0.0).astype(bf16)
            q2[pl.ds(n * ROWS, ROWS), :] = swap_halves(tile).astype(bf16)
            return carry

        lax.fori_loop(0, 8, prepare, 0)
        acc_p[...] = jnp.zeros_like(acc_p)
        acc_t[...] = jnp.zeros_like(acc_t)
        total_s[...] = jnp.zeros_like(total_s)
        carried_s[...] = jnp.zeros_like(carried_s)
        top_s[...] = jnp.full_like(top_s, NEG)

        def attend(block):
            keys = kv[t, block, :, 0:128]
            vals = kv[t, block, :, 128:256]
            nt = (((1,), (1,)), ((), ()))

            def chunk(i, carry):
                at = pl.ds(pl.multiple_of(i * 128, 128), 128)
                scores = lax.dot_general(q1[at, :], keys, nt, preferred_element_type=f32)
                tangs = lax.dot_general(q2[at, :], keys, nt, preferred_element_type=f32)
                old = top_s[at, :]
                new = jnp.maximum(old, jnp.max(scores, axis=-1, keepdims=True))
                fade = jnp.exp(old - new)
                top_s[at, :] = new
                weights_ = jnp.exp(scores - jnp.concatenate([new] * 4, axis=1))
                weighted = weights_ * tangs
                tot = fade * total_s[at, :]
                car = fade * carried_s[at, :]
                for k in range(4):
                    tot = tot + weights_[:, k * 128 : (k + 1) * 128]
                    car = car + weighted[:, k * 128 : (k + 1) * 128]
                total_s[at, :] = tot
                carried_s[at, :] = car
                acc_p[at, :] = fade * acc_p[at, :] + jnp.dot(
                    weights_.astype(bf16), vals, preferred_element_type=f32
                )
                acc_t[at, :] = fade * acc_t[at, :] + jnp.dot(
                    weighted.astype(bf16), vals, preferred_element_type=f32
                )
                return carry

            lax.fori_loop(0, 4, chunk, 0, unroll=True)

        attend(OWN)
        for p in (0, 1, 3, 2):
            part = relay.at[t, pl.ds(p * 128, 128)]
            remote(part, part, g_send.at[t, 0], r_recv.at[t, p], right).wait_recv()
            send(part, ZOWN, p, onward)
        for p in (0, 1):
            arrived(LEFT, p)
            send(piece(LEFT, p), FAR, p, right)
        for p in (3, 2):
            arrived(RIGHT, p)
            send(piece(RIGHT, p), FAR, p, left)
        arrived(LEFT, 3)
        arrived(LEFT, 2)
        attend(LEFT)
        arrived(RIGHT, 0)
        arrived(RIGHT, 1)
        attend(RIGHT)
        for p in (0, 1, 3, 2):
            arrived(ZOWN, p)
            send(piece(ZOWN, p), ZLEFT, p, right)
            send(piece(ZOWN, p), ZRIGHT, p, left)
        attend(ZOWN)
        for p in range(4):
            arrived(FAR, p)
        attend(FAR)
        for p in (0, 1):
            arrived(ZLEFT, p)
            send(piece(ZLEFT, p), ZFAR, p, right)
        for p in (3, 2):
            arrived(ZRIGHT, p)
            send(piece(ZRIGHT, p), ZFAR, p, left)
        arrived(ZLEFT, 3)
        arrived(ZLEFT, 2)
        attend(ZLEFT)
        arrived(ZRIGHT, 0)
        arrived(ZRIGHT, 1)
        attend(ZRIGHT)
        for p in range(4):
            arrived(ZFAR, p)
        attend(ZFAR)

        def finish(i, carry):
            at = pl.ds(pl.multiple_of(i * 128, 128), 128)
            total = jnp.sum(total_s[at, :], axis=-1, keepdims=True)
            carried = jnp.sum(carried_s[at, :], axis=-1, keepdims=True)
            ap = acc_p[at, :]
            prim = ap / total
            tang = (acc_t[at, :] + swap_halves(ap)) / total - (carried / total) * prim
            out = jnp.where(low_c, prim, swap_halves(tang)).astype(bf16)
            ret_stage[t, 2 * i] = out[:ROWS]
            ret_stage[t, 2 * i + 1] = out[ROWS:]
            return carry

        lax.fori_loop(0, 4, finish, 0)

        back = []
        for slot in (2, 1, 3, 0):
            for kind in (0, 1):
                n = slot * 2 + kind
                if n == 0:
                    continue
                m = ((4 - slot) % 4) * 2 + kind
                to = place(a + slot, g, z, c if kind == 0 else other)
                copy = remote(
                    ret_stage.at[t, n], ret.at[t, c, a], ret_send.at[t, n], ret_recv.at[t, m], to
                )
                copy.start()
                back.append(copy)
        ret_self = pltpu.make_async_copy(ret_stage.at[t, 0], ret.at[t, c, a], self_sem.at[2])
        ret_self.start()
        ret_self.wait()
        for m in range(1, 8):
            remote(
                ret_stage.at[t, 0], ret.at[t, 0, 0], ret_send.at[t, m], ret_recv.at[t, m], right
            ).wait_recv()

        def reduced_start(phase, at, value):
            red_send[t, phase, :, at] = value.astype(bf16)

        def reduce_copy(phase):
            return remote(
                red_send.at[t, phase], red_recv.at[t, phase], red_ssem.at[t, phase],
                red_rsem.at[t, phase], place(a, g, zpair, c),
            )

        def reduced(phase):
            return red_send[t, phase].astype(f32) + red_recv[t, phase].astype(f32)

        prims, tangs = [], []
        for cc in range(2):
            for j in range(2):
                first = ret[t, cc, 2 * j].astype(f32)
                second = ret[t, cc, 2 * j + 1].astype(f32)
                prims.append(jnp.where(low, first, swap_halves(second)).astype(bf16))
                tangs.append(jnp.where(low, swap_halves(first), second).astype(bf16))
        part = jnp.zeros((2 * ROWS, WIDTH), f32)
        for cc in range(2):
            heads = jnp.concatenate(
                [
                    jnp.concatenate(prims[2 * cc : 2 * cc + 2], axis=1),
                    jnp.concatenate(tangs[2 * cc : 2 * cc + 2], axis=1),
                ],
                axis=0,
            )
            part = part + jnp.dot(heads, wo[cc], preferred_element_type=f32)
        red_send[t, 0] = part.astype(bf16)
        first_sum = reduce_copy(0)
        first_sum.start()
        first_sum.wait()
        attn_s[...] = reduced(0)
        middle = inputs_s[...] + attn_s[:ROWS, :]
        middle_tang = direction[...] + attn_s[ROWS:, :]
        normed_s[...] = norm_pair(middle, middle_tang, gain_mlp[...])

        normed2 = normed_s[...]
        for cc in range(2):
            def hidden(j, carry):
                at = pl.ds(pl.multiple_of(j * 256, 256), 256)
                pre = jnp.dot(normed2, wi[cc, :, at], preferred_element_type=f32)
                act, act_tang = gelu_pair(pre[:ROWS], pre[ROWS:])
                act_s[cc, :ROWS, at] = act
                act_s[cc, ROWS:, at] = act_tang
                return carry

            lax.fori_loop(0, 4, hidden, 0)
        for j in range(4):
            at = slice(j * 256, (j + 1) * 256)
            red_send[t, 1, :, at] = (
                jnp.dot(act_s[0], wd[0, :, at], preferred_element_type=f32)
                + jnp.dot(act_s[1], wd[1, :, at], preferred_element_type=f32)
            ).astype(bf16)
        second_sum = reduce_copy(1)
        second_sum.start()
        second_sum.wait()
        field = attn_s[...] + reduced(1)
        trace_s[...] = trace_s[...] + jnp.sum(
            direction[...] * field[ROWS:], axis=-1, keepdims=True
        ) / (STEPS * WIDTH)
        state[...] = state[...] + field[:ROWS] / STEPS

        for copy in kv_out + q_out + sent + back:
            copy.wait_send()
        return carry

    lax.fori_loop(0, STEPS, one_step, 0)

    final = state[...]
    trace = trace_s[...]
    logp = (
        trace
        - 0.5 * jnp.sum(final * final, axis=-1, keepdims=True) / WIDTH
        - 0.5 * math.log(2.0 * math.pi)
    )
    stat_mine[0] = trace
    stat_mine[1] = logp
    spot = lax.broadcasted_iota(jnp.int32, (8, 128), 1) == s * 2 + c
    mean_send[0] = jnp.where(spot, jnp.sum(logp, axis=0, keepdims=True), 0.0)
    mine = pl.ds(row0, ROWS)
    finals = [
        remote(state, o_state.at[mine], fin_send.at[0], fin_recv.at[0], here),
        remote(stat_mine, stat_in, fin_send.at[1], fin_recv.at[1], here),
    ]
    for copy in finals:
        copy.start()
    o_state[mine, :] = final

    copies = []
    for d in range(4):
        slot = (4 - d) % 4
        for kind in range(2):
            if kind == 0 and d == 0:
                continue
            to = place(a + d, g, z, c) if kind == 0 else place(a, g + d, z, other)
            n = slot * 2 + kind
            copies.append(remote(
                mean_send.at[0], mean_recv.at[n], mean_ssem.at[n], mean_rsem.at[n], to
            ))
    for copy in copies:
        copy.start()
    for copy in copies:
        copy.wait()
    sum1 = mean_send[0]
    for n in range(1, 8):
        sum1 = sum1 + mean_recv[n]
    mean_send[1] = sum1
    copies = [
        remote(
            mean_send.at[1], mean_recv.at[7 + d], mean_ssem.at[7 + d], mean_rsem.at[7 + d],
            place(a, g + d, z, c),
        )
        for d in (1, 2, 3)
    ]
    for copy in copies:
        copy.start()
    for copy in copies:
        copy.wait()
    sum2 = (mean_send[1] + mean_recv[9]) + (mean_recv[8] + mean_recv[10])
    mean_send[2] = sum2
    last = remote(
        mean_send.at[2], mean_recv.at[11], mean_ssem.at[11], mean_rsem.at[11],
        place(a, g, z + 2, c),
    )
    last.start()
    last.wait()
    everyone = jnp.sum(mean_send[2] + mean_recv[11], axis=-1, keepdims=True)
    o_mean[...] = jnp.broadcast_to(everyone / (32 * SEQ_ROWS), (8, 128))

    for copy in finals:
        copy.wait()
    theirs = pl.ds(pl.multiple_of(other * ROWS, ROWS), ROWS)
    o_trace[mine, :] = stat_mine[0]
    o_logp[mine, :] = stat_mine[1]
    o_trace[theirs, :] = stat_in[0]
    o_logp[theirs, :] = stat_in[1]


def per_device(
    latent, probe, time_embed, gain_attn, w_query, w_key, w_value, w_out, gain_mlp, w_in, w_down
):
    hbm = pl.BlockSpec(memory_space=pl.ANY)
    vmem = pl.BlockSpec(memory_space=pltpu.VMEM)
    dma = pltpu.SemaphoreType.DMA
    T = STEPS
    state, trace, logp, mean = pl.pallas_call(
        kernel,
        out_shape=(
            jax.ShapeDtypeStruct((SEQ_ROWS, WIDTH), f32),
            jax.ShapeDtypeStruct((SEQ_ROWS, 128), f32),
            jax.ShapeDtypeStruct((SEQ_ROWS, 128), f32),
            jax.ShapeDtypeStruct((8, 128), f32),
        ),
        in_specs=[hbm, hbm, vmem, vmem, hbm, hbm, hbm, hbm, vmem, hbm, hbm],
        out_specs=(vmem, vmem, vmem, vmem),
        scratch_shapes=[
            pltpu.VMEM((ROWS, WIDTH), bf16),
            pltpu.VMEM((ROWS, WIDTH), bf16),
            pltpu.VMEM((2, WIDTH, 256), bf16),
            pltpu.VMEM((2, WIDTH, 256), bf16),
            pltpu.VMEM((2, WIDTH, 256), bf16),
            pltpu.VMEM((2, 256, WIDTH), bf16),
            pltpu.VMEM((2, WIDTH, WIDTH), bf16),
            pltpu.VMEM((2, WIDTH, WIDTH), bf16),
            pltpu.VMEM((ROWS, WIDTH), f32),
            pltpu.VMEM((ROWS, WIDTH), f32),
            pltpu.VMEM((ROWS, WIDTH), f32),
            pltpu.VMEM((ROWS, 128), f32),
            pltpu.VMEM((2 * ROWS, WIDTH), f32),
            pltpu.VMEM((2 * ROWS, WIDTH), bf16),
            pltpu.VMEM((2, 2 * ROWS, WIDTH), bf16),
            pltpu.VMEM((T, 2, 4, ROWS, 256), bf16),
            pltpu.VMEM((T, 2, 4, ROWS, 128), bf16),
            pltpu.VMEM((T, 8, QROWS, 256), bf16),
            pltpu.VMEM((T, 8, ROWS, 128), bf16),
            pltpu.VMEM((QROWS, 128), bf16),
            pltpu.VMEM((QROWS, 128), bf16),
            pltpu.VMEM((T, QROWS, 256), bf16),
            pltpu.VMEM((QROWS, 128), f32),
            pltpu.VMEM((QROWS, 128), f32),
            pltpu.VMEM((QROWS, 128), f32),
            pltpu.VMEM((QROWS, 128), f32),
            pltpu.VMEM((QROWS, 128), f32),
            pltpu.VMEM((T, 8, ROWS, 128), bf16),
            pltpu.VMEM((T, 2, 4, ROWS, 128), bf16),
            pltpu.VMEM((T, 2, 2 * ROWS, WIDTH), bf16),
            pltpu.VMEM((T, 2, 2 * ROWS, WIDTH), bf16),
            pltpu.VMEM((2, ROWS, 128), f32),
            pltpu.VMEM((2, ROWS, 128), f32),
            pltpu.VMEM((3, 8, 128), f32),
            pltpu.VMEM((12, 8, 128), f32),
            dma((8,)),
            dma((6,)),
            dma((6,)),
            dma((T, 8)),
            dma((T, 8)),
            dma((T, 8)),
            dma((T, 8)),
            dma((3,)),
            dma((T, 32)),
            dma((T, 8, 4)),
            dma((T, 4)),
            dma((T, 8)),
            dma((T, 8)),
            dma((T, 2)),
            dma((T, 2)),
            dma((2,)),
            dma((2,)),
            dma((12,)),
            dma((12,)),
        ],
        compiler_params=pltpu.CompilerParams(
            collective_id=0, has_side_effects=True, vmem_limit_bytes=60 * 1024 * 1024
        ),
        name="flow",
    )(
        latent, probe, time_embed.reshape(1, WIDTH), gain_attn.reshape(1, WIDTH), w_query, w_key,
        w_value, w_out, gain_mlp.reshape(1, WIDTH), w_in, w_down,
    )
    return (state, trace[:, 0], logp[:, 0], mean[0, 0])


def solution(mesh):
    return jax.shard_map(
        per_device,
        mesh=mesh,
        in_specs=(
            P("seq", None),
            P("seq", None),
            P(),
            P(),
            P(None, "head"),
            P(None, "head"),
            P(None, "head"),
            P("head", None),
            P(),
            P(None, "head"),
            P("head", None),
        ),
        out_specs=(P("seq", None), P("seq"), P("seq"), P()),
        check_vma=False,
    )
```

```python
import functools
import math

import jax
import jax.numpy as jnp
from jax import lax
from jax.experimental import pallas as pl
from jax.experimental.pallas import tpu as pltpu
from jax.sharding import PartitionSpec as P

HEAD_DIM = 64
STEPS = 2
EPSILON = 1e-05
GELU_COEF = 0.044715
ROOT_TWO_PI = math.sqrt(2.0 / math.pi)

ROWS = 64
SEQ_ROWS = 128
WIDTH = 1024
RING = 4
QROWS = 512
NEG = -1e30

CHUNK = 256

OWN, LEFT, RIGHT, FAR, ZOWN, ZLEFT, ZRIGHT, ZFAR = range(8)

f32 = jnp.float32
bf16 = jnp.bfloat16


def norm_pair(values, tangent, norm_gain):
    meansq = jnp.mean(values * values, axis=-1, keepdims=True) + EPSILON
    inverse = lax.rsqrt(meansq)
    inner_mean = jnp.mean(values * tangent, axis=-1, keepdims=True)
    primal = values * inverse * norm_gain
    derived = (tangent * inverse - values * inverse**3 * inner_mean) * norm_gain
    return jnp.concatenate([primal.astype(bf16), derived.astype(bf16)], axis=0)


def gelu_pair(pre_act, tangent):
    cubic_arg = pre_act + GELU_COEF * pre_act * pre_act * pre_act
    tanh_value = jnp.tanh(ROOT_TWO_PI * cubic_arg)
    output = 0.5 * pre_act * (1.0 + tanh_value)
    slope_value = 0.5 * (1.0 + tanh_value) + 0.5 * pre_act * (
        1.0 - tanh_value * tanh_value
    ) * ROOT_TWO_PI * (1.0 + 3.0 * GELU_COEF * pre_act * pre_act)
    return (output.astype(bf16), (slope_value * tangent).astype(bf16))


def swap_halves(tile):
    return pltpu.roll(tile, HEAD_DIM, 1)


def kernel(
    latent, probe, time_embed, gain_attn, w_query, w_key, w_value, w_out, gain_mlp, w_in, w_down,
    o_state, o_stats,
    lat_in, prb_in, wq, wk, wv, wo, wi, wd,
    state, direction, inputs_s, trace_s, attn_s, normed_s, act_s, probe_down,
    stage_kv, stage_q, kv, qin, q1, q2, acc_p, acc_t, top_s, total_s, carried_s,
    ret_stage, ret, red_send, red_recv, part_send, part_recv, stat_mine, stat_in,
    mean_send, mean_recv,
    load_sem, wsend, wrecv, out_send, out_recv, kv_send, kv_recv, q_send, q_recv, self_sem,
    g_send, g_recv, ret_send, ret_recv, red_ssem, red_rsem, fin_send, fin_recv,
    mean_ssem, mean_rsem,
):
    s = lax.axis_index("seq")
    hd = lax.axis_index("head")
    x = lax.rem(s // 4, 4)
    y = lax.rem(s, 4)
    c = lax.rem(hd, 2)
    other = 1 - c
    zlo = hd // 2
    z = (s // 16) * 2 + zlo
    a = y + c * (x - y)
    g = x + c * (y - x)

    def place(aa, gg, zz, cc):
        aa, gg, zz = lax.rem(aa, 4), lax.rem(gg, 4), lax.rem(zz, 4)
        xx = gg + c * (aa - gg)
        yy = aa + c * (gg - aa)
        return ((zz // 2) * 16 + xx * 4 + yy, lax.rem(zz, 2) * 2 + cc)

    def remote(src, dst, ssem, rsem, where):
        return pltpu.make_async_remote_copy(
            src_ref=src, dst_ref=dst, send_sem=ssem, recv_sem=rsem,
            device_id=where, device_id_type=pl.DeviceIdType.MESH,
        )

    here = place(a, g, z, other)
    zpair = z + 1 - 2 * zlo
    znext = z + 3 + 2 * zlo
    zfar = z + 2

    def both_ways(zz, first):
        return (
            [place(a + d, g, zz, c) for d in range(first, 4)]
            + [place(a + d, g, zz, other) for d in range(4)]
            + [place(a, g + d, zz, other) for d in (1, 2, 3)]
        )

    barrier = pltpu.get_barrier_semaphore()
    greeted = (
        both_ways(z, 1) + both_ways(zfar, 0) + both_ways(zpair, 0)
        + [place(a, g + d, z, c) for d in (1, 2, 3)]
        + [place(a, g + d, znext, c) for d in range(4)]
    )
    for where in greeted:
        pl.semaphore_signal(
            barrier, inc=1, device_id=where, device_id_type=pl.DeviceIdType.MESH
        )

    row0 = pl.multiple_of(c * ROWS, ROWS)
    loads = [
        pltpu.make_async_copy(latent.at[pl.ds(row0, ROWS)], lat_in, load_sem.at[0]),
        pltpu.make_async_copy(probe.at[pl.ds(row0, ROWS)], prb_in, load_sem.at[1]),
    ]
    weights = [(w_key, wk), (w_value, wv), (w_query, wq), (w_in, wi), (w_down, wd)]
    for i, (src, dst) in enumerate(weights):
        loads.append(pltpu.make_async_copy(src, dst.at[c], load_sem.at[2 + i]))
    loads.append(pltpu.make_async_copy(w_out, wo.at[hd], load_sem.at[7]))
    for load in loads:
        load.start()
    pl.semaphore_wait(barrier, len(greeted))
    swaps = [
        remote(src, dst.at[c], wsend.at[i], wrecv.at[i], here)
        for i, (src, dst) in enumerate(weights)
    ]
    out_here = remote(w_out, wo.at[hd], out_send.at[0], out_recv.at[0], here)
    out_pair = remote(
        w_out, wo.at[hd], out_send.at[1], out_recv.at[1], place(a, g, zpair, c)
    )
    pair_hd = 2 * (1 - zlo) + c
    out_on = remote(wo.at[pair_hd], wo.at[pair_hd], out_send.at[2], out_recv.at[2], here)
    for swap in swaps[:3] + [out_pair, out_here] + swaps[3:]:
        swap.start()

    loads[0].wait()
    loads[1].wait()
    state[...] = lat_in[...].astype(f32)
    direction[...] = prb_in[...].astype(f32)
    trace_s[...] = jnp.zeros_like(trace_s)

    lane = lax.broadcasted_iota(jnp.int32, (ROWS, 128), 1)
    low = lane < HEAD_DIM
    low_c = lax.broadcasted_iota(jnp.int32, (128, 128), 1) < HEAD_DIM
    low_t = lax.broadcasted_iota(jnp.int32, (8, 128), 1) < ROWS

    def weights_here(first, last):
        for i in range(first, last):
            loads[2 + i].wait()
            swaps[i].wait()

    def rows_to_lanes(first, second):
        tall = jnp.concatenate(
            [jnp.broadcast_to(first, (ROWS, 128)), jnp.broadcast_to(second, (ROWS, 128))], axis=0
        )
        return jnp.transpose(tall)[:8]

    def one_step(t, carry):
        inputs = state[...] + (t.astype(f32) / STEPS) * time_embed[...]
        inputs_s[...] = inputs
        normed_s[...] = norm_pair(inputs, direction[...], gain_attn[...])
        normed = normed_s[...]

        @pl.when(t == 0)
        def _():
            weights_here(0, 2)

        def project(weight, fill, scale):
            for cc in range(2):
                both = jnp.dot(normed, weight[cc], preferred_element_type=f32)
                if scale is not None:
                    both = both * scale
                for j in range(2):
                    prim = both[:ROWS, j * 128 : (j + 1) * 128]
                    tang = both[ROWS:, j * 128 : (j + 1) * 128]
                    fill(cc, 2 * j, jnp.where(low, prim, swap_halves(tang)).astype(bf16))
                    fill(cc, 2 * j + 1, jnp.where(low, swap_halves(prim), tang).astype(bf16))

        def kv_slot(block, slot, kind):
            return kv.at[t, block, pl.ds((slot * 2 + kind) * ROWS, ROWS)]

        def q_slot(slot, kind):
            return qin.at[t, slot * 2 + kind]

        def fill_key(cc, head, value):
            stage_kv[t, cc, head, :, :128] = value

        def fill_val(cc, head, value):
            stage_kv[t, cc, head, :, 128:] = value

        def fill_query(cc, head, value):
            stage_q[t, cc, head] = value

        project(wk, fill_key, None)
        project(wv, fill_val, None)

        kv_out, q_out = [], []
        for d in (2, 1, 3, 0):
            slot = (4 - d) % 4
            for kind in (1, 0):
                n = slot * 2 + kind
                if kind == 0:
                    cc, head = c, lax.rem(a + d, 4)
                else:
                    cc, head = other, lax.rem(g + d, 4)
                for block, zz, row in ((ZOWN, zfar, 1), (OWN, z, 0)):
                    to = place(a + d, g, zz, c) if kind == 0 else place(a, g + d, zz, other)
                    if n == 0 and block == OWN:
                        continue
                    copy = remote(
                        stage_kv.at[t, cc, head], kv_slot(block, slot, kind),
                        kv_send.at[t, row, n], kv_recv.at[t, row, n], to,
                    )
                    copy.start()
                    kv_out.append(copy)
        kv_self = pltpu.make_async_copy(stage_kv.at[t, c, a], kv_slot(OWN, 0, 0), self_sem.at[0])
        kv_self.start()

        @pl.when(t == 0)
        def _():
            weights_here(2, 3)

        project(wq, fill_query, HEAD_DIM**-0.5)
        for d in (2, 1, 3, 0):
            slot = (4 - d) % 4
            for kind in (1, 0):
                n = slot * 2 + kind
                if n == 0:
                    continue
                if kind == 0:
                    cc, head, to = c, lax.rem(a + d, 4), place(a + d, g, z, c)
                else:
                    cc, head, to = other, lax.rem(g + d, 4), place(a, g + d, z, other)
                copy = remote(
                    stage_q.at[t, cc, head], q_slot(slot, kind), q_send.at[t, n],
                    q_recv.at[t, n], to,
                )
                copy.start()
                q_out.append(copy)
        q_self = pltpu.make_async_copy(stage_q.at[t, c, a], q_slot(0, 0), self_sem.at[1])
        q_self.start()

        def piece(block, p):
            return kv.at[t, block, pl.ds(p * 128, 128)]

        sent = []

        def send(src, block, p, to):
            n = len(sent)
            copy = remote(src, piece(block, p), g_send.at[t, n], g_recv.at[t, block, p], to)
            copy.start()
            sent.append(copy)

        right, left = place(a, g + 1, z, c), place(a, g + 3, z, c)
        across = place(a, g + 2, z, c)

        def arrived(block, p):
            remote(
                piece(block, p), piece(block, p), g_send.at[t, 0], g_recv.at[t, block, p], right
            ).wait_recv()

        def slot_here(block, slot, row):
            for kind in range(2):
                n = slot * 2 + kind
                if n == 0 and block == OWN:
                    kv_self.wait()
                else:
                    part = kv_slot(block, slot, kind)
                    remote(
                        part, part, kv_send.at[t, row, n], kv_recv.at[t, row, n], right
                    ).wait_recv()

        for slot in (0, 1, 3, 2):
            slot_here(OWN, slot, 0)
            send(piece(OWN, slot), LEFT, slot, right)
            send(piece(OWN, slot), RIGHT, slot, left)

        def spread(slot):
            slot_here(ZOWN, slot, 1)
            send(piece(ZOWN, slot), ZFAR, slot, across)
            send(piece(ZOWN, slot), ZLEFT, slot, right)
            send(piece(ZOWN, slot), ZRIGHT, slot, left)

        for n in range(8):
            if n == 0:
                q_self.wait()
            else:
                remote(
                    qin.at[t, n], qin.at[t, n], q_send.at[t, n], q_recv.at[t, n], right
                ).wait_recv()

        def prepare(n, carry):
            tile = qin[t, n].astype(f32)
            q1[pl.ds(n * ROWS, ROWS), :] = jnp.where(low, tile, 0.0).astype(bf16)
            q2[pl.ds(n * ROWS, ROWS), :] = swap_halves(tile).astype(bf16)
            return carry

        lax.fori_loop(0, 8, prepare, 0)
        acc_p[...] = jnp.zeros_like(acc_p)
        acc_t[...] = jnp.zeros_like(acc_t)
        total_s[...] = jnp.zeros_like(total_s)
        carried_s[...] = jnp.zeros_like(carried_s)
        top_s[...] = jnp.full_like(top_s, NEG)

        def attend(block):
            keys = kv[t, block, :, 0:128]
            vals = kv[t, block, :, 128:256]
            nt = (((1,), (1,)), ((), ()))

            def chunk(i, carry):
                at = pl.ds(pl.multiple_of(i * CHUNK, CHUNK), CHUNK)
                both = lax.dot_general(
                    jnp.concatenate([q1[at, :], q2[at, :]], axis=0), keys, nt,
                    preferred_element_type=f32,
                )
                scores, tangs = both[:CHUNK], both[CHUNK:]
                old = top_s[at, :]
                new = jnp.maximum(old, jnp.max(scores, axis=-1, keepdims=True))
                fade = jnp.exp(old - new)
                top_s[at, :] = new
                weights_ = jnp.exp(scores - jnp.concatenate([new] * 4, axis=1))
                weighted = weights_ * tangs
                tot = fade * total_s[at, :]
                car = fade * carried_s[at, :]
                for k in range(4):
                    tot = tot + weights_[:, k * 128 : (k + 1) * 128]
                    car = car + weighted[:, k * 128 : (k + 1) * 128]
                total_s[at, :] = tot
                carried_s[at, :] = car
                out = jnp.dot(
                    jnp.concatenate([weights_.astype(bf16), weighted.astype(bf16)], axis=0), vals,
                    preferred_element_type=f32,
                )
                acc_p[at, :] = fade * acc_p[at, :] + out[:CHUNK]
                acc_t[at, :] = fade * acc_t[at, :] + out[CHUNK:]
                return carry

            lax.fori_loop(0, QROWS // CHUNK, chunk, 0, unroll=True)

        attend(OWN)
        spread(0)
        spread(1)
        for p in (0, 1):
            arrived(LEFT, p)
            send(piece(LEFT, p), FAR, p, right)
        for p in (3, 2):
            arrived(RIGHT, p)
            send(piece(RIGHT, p), FAR, p, left)
        arrived(LEFT, 3)
        arrived(LEFT, 2)
        attend(LEFT)
        spread(3)
        spread(2)
        arrived(RIGHT, 0)
        arrived(RIGHT, 1)
        attend(RIGHT)

        @pl.when(t == 0)
        def _():
            weights_here(3, 5)
            for cc in range(2):
                def down(j, carry):
                    at = pl.ds(pl.multiple_of(j * 256, 256), 256)
                    probe_down[cc, :, at] = lax.dot_general(
                        prb_in[...], wd[cc, at, :], (((1,), (1,)), ((), ())),
                        preferred_element_type=f32,
                    )
                    return carry

                lax.fori_loop(0, 4, down, 0)

        attend(ZOWN)
        for p in range(4):
            arrived(FAR, p)
        attend(FAR)

        @pl.when(t == 0)
        def _():
            loads[7].wait()
            out_pair.wait_recv()
            out_on.start()

        for block in (ZLEFT, ZRIGHT, ZFAR):
            for p in (0, 1, 3, 2):
                arrived(block, p)
            attend(block)

        def finish(i, carry):
            at = pl.ds(pl.multiple_of(i * 128, 128), 128)
            total = jnp.sum(total_s[at, :], axis=-1, keepdims=True)
            carried = jnp.sum(carried_s[at, :], axis=-1, keepdims=True)
            ap = acc_p[at, :]
            prim = ap / total
            tang = (acc_t[at, :] + swap_halves(ap)) / total - (carried / total) * prim
            out = jnp.where(low_c, prim, swap_halves(tang)).astype(bf16)
            ret_stage[t, 2 * i] = out[:ROWS]
            ret_stage[t, 2 * i + 1] = out[ROWS:]
            return carry

        lax.fori_loop(0, 4, finish, 0)

        back = []
        for slot in (2, 1, 3, 0):
            for kind in (0, 1):
                n = slot * 2 + kind
                m = ((4 - slot) % 4) * 2 + kind
                for row, zz in ((1, zpair), (0, z)):
                    if n == 0 and row == 0:
                        continue
                    copy = remote(
                        ret_stage.at[t, n], ret.at[t, hd, a], ret_send.at[t, row, n],
                        ret_recv.at[t, row, m], place(a + slot, g, zz, c if kind == 0 else other),
                    )
                    copy.start()
                    back.append(copy)
        ret_self = pltpu.make_async_copy(ret_stage.at[t, 0], ret.at[t, hd, a], self_sem.at[2])
        ret_self.start()

        @pl.when(t == 0)
        def _():
            out_here.wait()
            out_pair.wait_send()
            out_on.wait()

        ret_self.wait()
        for row in range(2):
            for m in range(8):
                if m == 0 and row == 0:
                    continue
                remote(
                    ret_stage.at[t, 0], ret.at[t, 0, 0], ret_send.at[t, row, m],
                    ret_recv.at[t, row, m], right,
                ).wait_recv()

        prims, tangs = [], []
        for cc in range(4):
            for j in range(2):
                first = ret[t, cc, 2 * j].astype(f32)
                second = ret[t, cc, 2 * j + 1].astype(f32)
                prims.append(jnp.where(low, first, swap_halves(second)).astype(bf16))
                tangs.append(jnp.where(low, swap_halves(first), second).astype(bf16))
        part = jnp.zeros((2 * ROWS, WIDTH), f32)
        for cc in range(4):
            heads = jnp.concatenate(
                [
                    jnp.concatenate(prims[2 * cc : 2 * cc + 2], axis=1),
                    jnp.concatenate(tangs[2 * cc : 2 * cc + 2], axis=1),
                ],
                axis=0,
            )
            part = part + jnp.dot(heads, wo[cc], preferred_element_type=f32)
        attn_s[...] = part
        middle = inputs_s[...] + attn_s[:ROWS, :]
        middle_tang = direction[...] + attn_s[ROWS:, :]
        normed_s[...] = norm_pair(middle, middle_tang, gain_mlp[...])

        normed2 = normed_s[...]
        part_s = jnp.zeros((ROWS, 256), f32)
        for cc in range(2):
            for j in range(4):
                at = slice(j * 256, (j + 1) * 256)
                pre = jnp.dot(normed2, wi[cc, :, at], preferred_element_type=f32)
                act, act_tang = gelu_pair(pre[:ROWS], pre[ROWS:])
                act_s[cc, :, at] = act
                part_s = part_s + act_tang.astype(f32) * probe_down[cc, :, at]
        pair = place(a, g, zpair, c)
        sums = []
        for j in range(4):
            at = slice(j * 256, (j + 1) * 256)
            red_send[t, j] = (
                jnp.dot(act_s[0], wd[0, :, at], preferred_element_type=f32)
                + jnp.dot(act_s[1], wd[1, :, at], preferred_element_type=f32)
            ).astype(bf16)
            copy = remote(
                red_send.at[t, j], red_recv.at[t, j], red_ssem.at[t, j], red_rsem.at[t, j], pair
            )
            copy.start()
            sums.append(copy)
        part_send[t] = rows_to_lanes(
            jnp.sum(part_s, axis=-1, keepdims=True),
            jnp.sum(direction[...] * attn_s[ROWS:, :], axis=-1, keepdims=True),
        )
        copy = remote(
            part_send.at[t], part_recv.at[t], red_ssem.at[t, 4], red_rsem.at[t, 4], pair
        )
        copy.start()
        for j, summed in enumerate(sums):
            at = slice(j * 256, (j + 1) * 256)
            summed.wait()
            mlp = red_send[t, j].astype(f32) + red_recv[t, j].astype(f32)
            state[:, at] = state[:, at] + (attn_s[:ROWS, at] + mlp) / STEPS
        copy.wait()
        share = part_send[t]
        trace_s[...] = trace_s[...] + (
            (share + part_recv[t]) + pltpu.roll(share, ROWS, 1)
        ) / (STEPS * WIDTH)

        for copy in kv_out + q_out + sent + back:
            copy.wait_send()
        return carry

    lax.fori_loop(0, STEPS, one_step, 0)

    final = state[...]
    squares = jnp.sum(final * final, axis=-1, keepdims=True)
    trace = trace_s[...]
    logp = (
        trace - 0.5 * rows_to_lanes(squares, squares) / WIDTH - 0.5 * math.log(2.0 * math.pi)
    )
    trace = jnp.where(low_t, trace, 0.0)
    logp = jnp.where(low_t, logp, 0.0)
    first = c == 0
    stat_mine[0] = jnp.where(first, trace, pltpu.roll(trace, ROWS, 1))
    stat_mine[1] = jnp.where(first, logp, pltpu.roll(logp, ROWS, 1))
    spot = lax.broadcasted_iota(jnp.int32, (8, 128), 1) == s * 2 + c
    mean_send[0] = jnp.where(spot, jnp.sum(logp, axis=-1, keepdims=True), 0.0)
    mine = pl.ds(row0, ROWS)
    finals = [
        remote(state, o_state.at[mine], fin_send.at[0], fin_recv.at[0], here),
        remote(stat_mine, stat_in, fin_send.at[1], fin_recv.at[1], here),
    ]
    for copy in finals:
        copy.start()
    o_state[mine, :] = final

    copies = []
    for d in range(4):
        slot = (4 - d) % 4
        for kind in range(2):
            if kind == 0 and d == 0:
                continue
            to = place(a + d, g, z, c) if kind == 0 else place(a, g + d, z, other)
            n = slot * 2 + kind
            copies.append(remote(
                mean_send.at[0], mean_recv.at[n], mean_ssem.at[n], mean_rsem.at[n], to
            ))
    for copy in copies:
        copy.start()
    for copy in copies:
        copy.wait()
    sum1 = mean_send[0]
    for n in range(1, 8):
        sum1 = sum1 + mean_recv[n]
    mean_send[1] = sum1
    copies = []
    for row, zz in ((1, znext), (0, z)):
        for d in (2, 1, 3, 0):
            if d == 0 and row == 0:
                continue
            n = 8 + row * 4 + d
            copies.append(remote(
                mean_send.at[1], mean_recv.at[n], mean_ssem.at[n], mean_rsem.at[n],
                place(a, g + d, zz, c),
            ))
    for copy in copies:
        copy.start()
    for copy in copies:
        copy.wait()
    everyone = mean_send[1]
    for n in range(9, 16):
        everyone = everyone + mean_recv[n]
    everyone = jnp.sum(everyone, axis=-1, keepdims=True)
    o_stats[2] = jnp.broadcast_to(everyone / (32 * SEQ_ROWS), (8, 128))
    for copy in finals:
        copy.wait()
    o_stats[0] = stat_mine[0] + stat_in[0]
    o_stats[1] = stat_mine[1] + stat_in[1]


def write_out(state, stats, o_state, o_trace, o_logp, o_mean):
    o_state[...] = state[...]
    o_trace[...] = stats[0, 0:1, :]
    o_logp[...] = stats[1, 0:1, :]
    o_mean[...] = stats[2, 0:1, 0:1]


def per_device(
    latent, probe, time_embed, gain_attn, w_query, w_key, w_value, w_out, gain_mlp, w_in, w_down
):
    hbm = pl.BlockSpec(memory_space=pl.ANY)
    vmem = pl.BlockSpec(memory_space=pltpu.VMEM)
    dma = pltpu.SemaphoreType.DMA
    T = STEPS
    state, stats = pl.pallas_call(
        kernel,
        out_shape=(
            jax.ShapeDtypeStruct((SEQ_ROWS, WIDTH), f32),
            jax.ShapeDtypeStruct((3, 8, 128), f32),
        ),
        in_specs=[hbm, hbm, vmem, vmem, hbm, hbm, hbm, hbm, vmem, hbm, hbm],
        out_specs=(vmem, vmem),
        scratch_shapes=[
            pltpu.VMEM((ROWS, WIDTH), bf16),
            pltpu.VMEM((ROWS, WIDTH), bf16),
            pltpu.VMEM((2, WIDTH, 256), bf16),
            pltpu.VMEM((2, WIDTH, 256), bf16),
            pltpu.VMEM((2, WIDTH, 256), bf16),
            pltpu.VMEM((4, 256, WIDTH), bf16),
            pltpu.VMEM((2, WIDTH, WIDTH), bf16),
            pltpu.VMEM((2, WIDTH, WIDTH), bf16),
            pltpu.VMEM((ROWS, WIDTH), f32),
            pltpu.VMEM((ROWS, WIDTH), f32),
            pltpu.VMEM((ROWS, WIDTH), f32),
            pltpu.VMEM((8, 128), f32),
            pltpu.VMEM((2 * ROWS, WIDTH), f32),
            pltpu.VMEM((2 * ROWS, WIDTH), bf16),
            pltpu.VMEM((2, ROWS, WIDTH), bf16),
            pltpu.VMEM((2, ROWS, WIDTH), f32),
            pltpu.VMEM((T, 2, 4, ROWS, 256), bf16),
            pltpu.VMEM((T, 2, 4, ROWS, 128), bf16),
            pltpu.VMEM((T, 8, QROWS, 256), bf16),
            pltpu.VMEM((T, 8, ROWS, 128), bf16),
            pltpu.VMEM((QROWS, 128), bf16),
            pltpu.VMEM((QROWS, 128), bf16),
            pltpu.VMEM((QROWS, 128), f32),
            pltpu.VMEM((QROWS, 128), f32),
            pltpu.VMEM((QROWS, 128), f32),
            pltpu.VMEM((QROWS, 128), f32),
            pltpu.VMEM((QROWS, 128), f32),
            pltpu.VMEM((T, 8, ROWS, 128), bf16),
            pltpu.VMEM((T, 4, 4, ROWS, 128), bf16),
            pltpu.VMEM((T, 4, ROWS, 256), bf16),
            pltpu.VMEM((T, 4, ROWS, 256), bf16),
            pltpu.VMEM((T, 8, 128), f32),
            pltpu.VMEM((T, 8, 128), f32),
            pltpu.VMEM((2, 8, 128), f32),
            pltpu.VMEM((2, 8, 128), f32),
            pltpu.VMEM((2, 8, 128), f32),
            pltpu.VMEM((16, 8, 128), f32),
            dma((8,)),
            dma((5,)),
            dma((5,)),
            dma((3,)),
            dma((3,)),
            dma((T, 2, 8)),
            dma((T, 2, 8)),
            dma((T, 8)),
            dma((T, 8)),
            dma((3,)),
            dma((T, 24)),
            dma((T, 8, 4)),
            dma((T, 2, 8)),
            dma((T, 2, 8)),
            dma((T, 5)),
            dma((T, 5)),
            dma((2,)),
            dma((2,)),
            dma((16,)),
            dma((16,)),
        ],
        compiler_params=pltpu.CompilerParams(
            collective_id=0, has_side_effects=True, vmem_limit_bytes=60 * 1024 * 1024
        ),
        name="flow",
    )(
        latent, probe, time_embed.reshape(1, WIDTH), gain_attn.reshape(1, WIDTH), w_query, w_key,
        w_value, w_out, gain_mlp.reshape(1, WIDTH), w_in, w_down,
    )
    state, trace, logp, mean = pl.pallas_call(
        write_out,
        out_shape=(
            jax.ShapeDtypeStruct((SEQ_ROWS, WIDTH), f32),
            jax.ShapeDtypeStruct((1, SEQ_ROWS), f32),
            jax.ShapeDtypeStruct((1, SEQ_ROWS), f32),
            jax.ShapeDtypeStruct((1, 1), f32),
        ),
        in_specs=[vmem, vmem],
        out_specs=(vmem, vmem, vmem, vmem),
        name="write_out",
    )(state, stats)
    return (state, trace.reshape(SEQ_ROWS), logp.reshape(SEQ_ROWS), mean.reshape(()))


def solution(mesh):
    return jax.shard_map(
        per_device,
        mesh=mesh,
        in_specs=(
            P("seq", None),
            P("seq", None),
            P(),
            P(),
            P(None, "head"),
            P(None, "head"),
            P(None, "head"),
            P("head", None),
            P(),
            P(None, "head"),
            P("head", None),
        ),
        out_specs=(P("seq", None), P("seq"), P("seq"), P()),
        check_vma=False,
    )
```
